32 devices in a mesh: grp: 4 (over z), dev: 8 (over y, x, core).
Axes of the slice: x: 2, y: 2, z: 4, core: 2. Of those that a mesh axis runs over, the one named last changes fastest.
Arguments:
- amounts: float32 [64, 524288], P('dev', 'grp'), may hold values from -0.06 to 0.06, as said below
Outputs:
- offsets: float32 [64, 524288], P(None, ('grp', 'dev'))
The draws below stay inside these ranges and needn't reach their ends.
Inputs may be any that keep to these rules, and one draw needn't show every extreme that they name: `amounts`: each entry lies within 0.06 of zero.
All inputs are finite; a program needn't handle non-finite values.
Results may differ from the reference program's by a relative error of at most 0.00095.
Values sent between devices are 32-bit elements; how exact they have to be, the bound alone decides.
A program may use at most 64 MiB of HBM per device.

```python
import jax
import jax.numpy as jnp

COLS = 64
ROW_DEV = 16384
ROWS = 524288


def draw_amounts(key, part):
    subkeys = jax.random.split(jax.random.fold_in(key, 17), 3)
    regions = ROWS // (ROW_DEV // 4)
    noise = jax.random.uniform(subkeys[0], (COLS, ROWS + 1), jnp.float32, -1.0, 1.0)
    reach = 1.0
    drift = jax.random.uniform(subkeys[2], (COLS, 1), jnp.float32, 0.0, 2.0)
    factor = jnp.exp(jax.random.uniform(subkeys[1], (COLS, regions), jnp.float32, -reach, reach))
    factor = jnp.repeat(factor, ROW_DEV // 4, axis=1, total_repeat_length=ROWS)
    rough = 0.01 * (noise[:, 1:] - noise[:, :-1])
    values = factor * (rough + drift / ROWS)
    return values.astype(jnp.float32)


def setup_inputs(seed: int = 0) -> dict:
    arg_keys = jax.random.split(jax.random.key(seed), 2)
    amounts = draw_amounts(jax.random.fold_in(arg_keys[1], 71), 0)
    return {"amounts": amounts}


def exclusive_rows(values, block_len):
    chans, length = values.shape
    blocks = values.reshape(chans, length // block_len, block_len)
    within = jnp.cumsum(blocks, axis=2) - blocks
    sums = jnp.sum(blocks, axis=2)
    starts = jnp.cumsum(sums, axis=1) - sums
    return (within + starts[:, :, None]).reshape(chans, length)


def reference(amounts):
    return exclusive_rows(amounts, 512)
```

```python
import functools

import jax
import jax.numpy as jnp
from jax import lax
from jax.experimental import pallas as pl
from jax.experimental.pallas import tpu as pltpu
from jax.sharding import PartitionSpec as P

MESH = pl.DeviceIdType.MESH
LANES = 128


def partner(me, k, n):
    if n & (n - 1):
        return lax.rem(me + k, n)
    other, bit = me, 1
    while bit < n:
        if k & bit:
            other = other + bit - 2 * bit * lax.rem(me // bit, 2)
        bit *= 2
    return other


def visit_order(n):
    return [*range(2, n, 2), *range(3, n, 2), *range(1, min(n, 2)), 0]


def piece_spans(rows):
    cuts = [0, rows // 8, rows // 4, rows // 2, rows]
    return list(zip(cuts[:-1], cuts[1:]))


def kernel(n, groups, x_ref, t_ref, carry_ref, x_vm, s_vm, w_vm, run_vm, group_vm, give_vm,
           load_sem, send_sem, recv_sem, csend_sem, crecv_sem, zsend_sem, zrecv_sem):
    me, grp = lax.axis_index("dev"), lax.axis_index("grp")
    chans, rows = t_ref.shape[1:]
    order = visit_order(n)
    spans = piece_spans(rows)
    others = {k: partner(me, k, n) for k in order}

    barrier = pltpu.get_barrier_semaphore()
    for k in order:
        if k:
            pl.semaphore_signal(barrier, inc=1, device_id={"dev": others[k]}, device_id_type=MESH)

    @pl.when(grp > 0)
    def _():
        pl.semaphore_signal(barrier, inc=1, device_id={"grp": grp - 1}, device_id_type=MESH)

    @pl.when(grp < groups - 1)
    def _():
        pl.semaphore_signal(barrier, inc=1, device_id={"grp": grp + 1}, device_id_type=MESH)

    def load(piece, k):
        lo, hi = spans[piece]
        at = pl.ds(pl.multiple_of(others[k] * rows + lo, LANES), hi - lo)
        return pltpu.make_async_copy(x_ref.at[:, at], x_vm.at[:, at], load_sem.at[piece, k])

    for piece in range(len(spans)):
        for k in order:
            load(piece, k).start()

    shape = (2 * LANES, 2 * LANES)
    row = lax.rem(lax.broadcasted_iota(jnp.int32, shape, 0), LANES)
    col = lax.broadcasted_iota(jnp.int32, shape, 1)
    w_vm[...] = jnp.where((row < col) | (col >= LANES), 1.0, 0.0).astype(jnp.bfloat16)
    run_vm[...] = jnp.zeros_like(run_vm)

    tile = min(rows // 8, 2048)
    steps = tile // LANES

    def scan(piece, k):
        lo, hi = spans[piece]
        base = others[k] * rows
        dest = t_ref.at[me] if k == 0 else s_vm.at[others[k]]

        def one(i, run):
            start = lo + i * tile
            block = x_vm[:, pl.ds(pl.multiple_of(base + start, LANES), tile)]
            stack = jnp.concatenate(
                [block[:, j * LANES:(j + 1) * LANES] for j in range(steps)], axis=0)
            high = stack.astype(jnp.bfloat16)
            rest = stack - high.astype(jnp.float32)
            mid = rest.astype(jnp.bfloat16)
            low = (rest - mid.astype(jnp.float32)).astype(jnp.bfloat16)
            sums = jnp.dot(jnp.concatenate([high, mid], axis=1), w_vm[...],
                           preferred_element_type=jnp.float32)
            sums = sums + jnp.dot(low, w_vm[:LANES, :], preferred_element_type=jnp.float32)
            for j in range(steps):
                part = sums[j * chans:(j + 1) * chans]
                at = pl.ds(pl.multiple_of(start + j * LANES, LANES), LANES)
                dest[:, at] = part[:, :LANES] + run
                run = run + part[:, LANES:]
            return run

        run_vm[others[k]] = lax.fori_loop(0, (hi - lo) // tile, one, run_vm[others[k]])

    def send(piece, k):
        lo, hi = spans[piece]
        at = pl.ds(lo, hi - lo)
        pltpu.make_async_remote_copy(
            src_ref=s_vm.at[others[k], :, at], dst_ref=t_ref.at[me, :, at],
            send_sem=send_sem.at[others[k]], recv_sem=recv_sem.at[me],
            device_id={"dev": others[k]}, device_id_type=MESH).start()

    near = jnp.where(grp > 0, 1, 0) + jnp.where(grp < groups - 1, 1, 0)
    late = None
    for piece in range(len(spans)):
        for k in order:
            load(piece, k).wait()
            scan(piece, k)
            if late is None and piece == 0:
                pl.semaphore_wait(barrier, n - 1 + near)
            if late is not None:
                send(*late)
            late = (piece, k) if k else None

    total = jnp.zeros((chans, LANES), jnp.float32)
    for j in range(n):
        give_vm[j] = total
        total = total + run_vm[j]

    def pass_on():
        return pltpu.make_async_remote_copy(
            src_ref=group_vm.at[1], dst_ref=group_vm.at[0], send_sem=zsend_sem, recv_sem=zrecv_sem,
            device_id={"grp": grp + 1}, device_id_type=MESH)

    @pl.when(grp == 0)
    def _():
        group_vm[0] = jnp.zeros_like(total)

    @pl.when(grp > 0)
    def _():
        pass_on().wait_recv()

    before = group_vm[0]
    group_vm[1] = before + total
    for j in range(n):
        give_vm[j] = give_vm[j] + before
    carry_ref[me] = give_vm[me]

    @pl.when(grp < groups - 1)
    def _():
        pass_on().start()

    def give(k, source):
        return pltpu.make_async_remote_copy(
            src_ref=give_vm.at[others[k]], dst_ref=carry_ref.at[source],
            send_sem=csend_sem.at[others[k]], recv_sem=crecv_sem.at[source],
            device_id={"dev": others[k]}, device_id_type=MESH)

    for k in order:
        if k:
            give(k, me).start()

    @pl.when(grp < groups - 1)
    def _():
        pass_on().wait_send()

    for k in order:
        if k:
            pltpu.make_async_remote_copy(
                src_ref=s_vm.at[others[k]], dst_ref=t_ref.at[others[k]],
                send_sem=send_sem.at[others[k]], recv_sem=recv_sem.at[others[k]],
                device_id={"dev": others[k]}, device_id_type=MESH).wait()
            give(k, others[k]).wait()


def solution(mesh):
    n, groups = mesh.shape["dev"], mesh.shape["grp"]

    def local(amounts):
        chans, length = amounts.shape
        rows = length // n
        f32 = jnp.float32
        table, carry = pl.pallas_call(
            functools.partial(kernel, n, groups),
            out_shape=[jax.ShapeDtypeStruct((n, chans, rows), f32),
                       jax.ShapeDtypeStruct((n, chans, LANES), f32)],
            in_specs=[pl.BlockSpec(memory_space=pl.ANY)],
            out_specs=[pl.BlockSpec(memory_space=pltpu.VMEM)] * 2,
            scratch_shapes=[
                pltpu.VMEM((chans, length), f32),
                pltpu.VMEM((n, chans, rows), f32),
                pltpu.VMEM((2 * LANES, 2 * LANES), jnp.bfloat16),
                pltpu.VMEM((n, chans, LANES), f32),
                pltpu.VMEM((2, chans, LANES), f32),
                pltpu.VMEM((n, chans, LANES), f32),
                pltpu.SemaphoreType.DMA((len(piece_spans(rows)), n)),
                pltpu.SemaphoreType.DMA((n,)),
                pltpu.SemaphoreType.DMA((n,)),
                pltpu.SemaphoreType.DMA((n,)),
                pltpu.SemaphoreType.DMA((n,)),
                pltpu.SemaphoreType.DMA,
                pltpu.SemaphoreType.DMA,
            ],
            compiler_params=pltpu.CompilerParams(collective_id=0, has_side_effects=True),
            name="exchange",
        )(amounts)
        return (table + carry[:, :, :1]).reshape(n * chans, rows)

    return jax.shard_map(
        local,
        mesh=mesh,
        in_specs=(P("dev", "grp"),),
        out_specs=P(None, ("grp", "dev")),
        check_vma=False,
    )
```

```python
import functools

import jax
import jax.numpy as jnp
from jax import lax
from jax.experimental import pallas as pl
from jax.experimental.pallas import tpu as pltpu
from jax.sharding import PartitionSpec as P

MESH = pl.DeviceIdType.MESH
LANES = 128
VMEM_GRANT = 46 << 20


def partner(me, k, n):
    if n & (n - 1):
        return lax.rem(me + k, n)
    other, bit = me, 1
    while bit < n:
        if k & bit:
            other = other + bit - 2 * bit * lax.rem(me // bit, 2)
        bit *= 2
    return other


def visit_order(n):
    return [*range(2, n, 2), *range(3, n, 2), *range(1, min(n, 2)), 0]


def piece_spans(rows):
    cuts = [0, rows // 8, rows // 4, rows // 2, rows]
    return list(zip(cuts[:-1], cuts[1:]))


def kernel(n, groups, x_ref, t_ref, carry_ref, x_vm, s_vm, w_vm, run_vm, group_vm, give_vm,
           load_sem, send_sem, recv_sem, csend_sem, crecv_sem, zsend_sem, zrecv_sem):
    me, grp = lax.axis_index("dev"), lax.axis_index("grp")
    chans, rows = t_ref.shape[1:]
    order = visit_order(n)
    spans = piece_spans(rows)
    others = {k: partner(me, k, n) for k in order}

    barrier = pltpu.get_barrier_semaphore()
    for k in order:
        if k:
            pl.semaphore_signal(barrier, inc=1, device_id={"dev": others[k]}, device_id_type=MESH)

    @pl.when(grp > 0)
    def _():
        pl.semaphore_signal(barrier, inc=1, device_id={"grp": grp - 1}, device_id_type=MESH)

    @pl.when(grp < groups - 1)
    def _():
        pl.semaphore_signal(barrier, inc=1, device_id={"grp": grp + 1}, device_id_type=MESH)

    def load(piece, k):
        lo, hi = spans[piece]
        at = pl.ds(pl.multiple_of(others[k] * rows + lo, LANES), hi - lo)
        return pltpu.make_async_copy(x_ref.at[:, at], x_vm.at[:, at], load_sem.at[piece, k])

    for piece in range(len(spans)):
        for k in order:
            load(piece, k).start()

    shape = (2 * LANES, 2 * LANES)
    row = lax.rem(lax.broadcasted_iota(jnp.int32, shape, 0), LANES)
    col = lax.broadcasted_iota(jnp.int32, shape, 1)
    w_vm[...] = jnp.where((row < col) | (col >= LANES), 1.0, 0.0).astype(jnp.bfloat16)
    run_vm[...] = jnp.zeros_like(run_vm)

    tile = min(rows // 8, 2048)
    steps = tile // LANES

    def scan(piece, k):
        lo, hi = spans[piece]
        base = others[k] * rows
        dest = t_ref.at[me] if k == 0 else s_vm.at[others[k]]

        def one(i, run):
            start = lo + i * tile
            block = x_vm[:, pl.ds(pl.multiple_of(base + start, LANES), tile)]
            stack = jnp.concatenate(
                [block[:, j * LANES:(j + 1) * LANES] for j in range(steps)], axis=0)
            high = stack.astype(jnp.bfloat16)
            rest = stack - high.astype(jnp.float32)
            mid = rest.astype(jnp.bfloat16)
            low = (rest - mid.astype(jnp.float32)).astype(jnp.bfloat16)
            sums = jnp.dot(jnp.concatenate([high, mid], axis=1), w_vm[...],
                           preferred_element_type=jnp.float32)
            sums = sums + jnp.dot(low, w_vm[:LANES, :], preferred_element_type=jnp.float32)
            for j in range(steps):
                part = sums[j * chans:(j + 1) * chans]
                at = pl.ds(pl.multiple_of(start + j * LANES, LANES), LANES)
                dest[:, at] = part[:, :LANES] + run
                run = run + part[:, LANES:]
            return run

        run_vm[others[k]] = lax.fori_loop(0, (hi - lo) // tile, one, run_vm[others[k]])

    def send(piece, k):
        lo, hi = spans[piece]
        at = pl.ds(lo, hi - lo)
        pltpu.make_async_remote_copy(
            src_ref=s_vm.at[others[k], :, at], dst_ref=t_ref.at[me, :, at],
            send_sem=send_sem.at[others[k]], recv_sem=recv_sem.at[me],
            device_id={"dev": others[k]}, device_id_type=MESH).start()

    near = jnp.where(grp > 0, 1, 0) + jnp.where(grp < groups - 1, 1, 0)
    late = None
    for piece in range(len(spans)):
        for k in order:
            load(piece, k).wait()
            scan(piece, k)
            if late is None and piece == 0:
                pl.semaphore_wait(barrier, n - 1 + near)
            if late is not None:
                send(*late)
            late = (piece, k) if k else None

    total = jnp.zeros((chans, LANES), jnp.float32)
    for j in range(n):
        give_vm[j] = total
        total = total + run_vm[j]

    def pass_on():
        return pltpu.make_async_remote_copy(
            src_ref=group_vm.at[1], dst_ref=group_vm.at[0], send_sem=zsend_sem, recv_sem=zrecv_sem,
            device_id={"grp": grp + 1}, device_id_type=MESH)

    @pl.when(grp == 0)
    def _():
        group_vm[0] = jnp.zeros_like(total)

    @pl.when(grp > 0)
    def _():
        pass_on().wait_recv()

    before = group_vm[0]
    group_vm[1] = before + total
    for j in range(n):
        give_vm[j] = give_vm[j] + before
    carry_ref[me] = give_vm[me]

    @pl.when(grp < groups - 1)
    def _():
        pass_on().start()

    def give(k, source):
        return pltpu.make_async_remote_copy(
            src_ref=give_vm.at[others[k]], dst_ref=carry_ref.at[source],
            send_sem=csend_sem.at[others[k]], recv_sem=crecv_sem.at[source],
            device_id={"dev": others[k]}, device_id_type=MESH)

    for k in order:
        if k:
            give(k, me).start()

    @pl.when(grp < groups - 1)
    def _():
        pass_on().wait_send()

    for k in order:
        if k:
            pltpu.make_async_remote_copy(
                src_ref=s_vm.at[others[k]], dst_ref=t_ref.at[others[k]],
                send_sem=send_sem.at[others[k]], recv_sem=recv_sem.at[others[k]],
                device_id={"dev": others[k]}, device_id_type=MESH).wait()
            give(k, others[k]).wait()


def finish(n, t_ref, carry_ref, out_ref, stage, sem):
    rows = t_ref.shape[2]
    step = min(rows, 16 * LANES)

    def copy(j):
        return pltpu.make_async_copy(stage.at[j], out_ref.at[j], sem.at[j])

    for j in range(n):
        carry = carry_ref[j]
        wide = jnp.concatenate([carry] * (step // LANES), axis=1)

        def add(i, _):
            at = pl.ds(pl.multiple_of(i * step, LANES), step)
            stage[j, :, at] = t_ref[j, :, at] + wide
            return 0

        lax.fori_loop(0, rows // step, add, 0, unroll=True)
        copy(j).start()
    for j in range(n):
        copy(j).wait()


def solution(mesh):
    n, groups = mesh.shape["dev"], mesh.shape["grp"]

    def local(amounts):
        chans, length = amounts.shape
        rows = length // n
        f32 = jnp.float32
        table, carry = pl.pallas_call(
            functools.partial(kernel, n, groups),
            out_shape=[jax.ShapeDtypeStruct((n, chans, rows), f32),
                       jax.ShapeDtypeStruct((n, chans, LANES), f32)],
            in_specs=[pl.BlockSpec(memory_space=pl.ANY)],
            out_specs=[pl.BlockSpec(memory_space=pltpu.VMEM)] * 2,
            scratch_shapes=[
                pltpu.VMEM((chans, length), f32),
                pltpu.VMEM((n, chans, rows), f32),
                pltpu.VMEM((2 * LANES, 2 * LANES), jnp.bfloat16),
                pltpu.VMEM((n, chans, LANES), f32),
                pltpu.VMEM((2, chans, LANES), f32),
                pltpu.VMEM((n, chans, LANES), f32),
                pltpu.SemaphoreType.DMA((len(piece_spans(rows)), n)),
                pltpu.SemaphoreType.DMA((n,)),
                pltpu.SemaphoreType.DMA((n,)),
                pltpu.SemaphoreType.DMA((n,)),
                pltpu.SemaphoreType.DMA((n,)),
                pltpu.SemaphoreType.DMA,
                pltpu.SemaphoreType.DMA,
            ],
            compiler_params=pltpu.CompilerParams(
                collective_id=0, has_side_effects=True, vmem_limit_bytes=VMEM_GRANT),
            name="exchange",
        )(amounts)
        out = pl.pallas_call(
            functools.partial(finish, n),
            out_shape=jax.ShapeDtypeStruct((n, chans, rows), f32),
            in_specs=[pl.BlockSpec(memory_space=pltpu.VMEM)] * 2,
            out_specs=pl.BlockSpec(memory_space=pl.ANY),
            scratch_shapes=[
                pltpu.VMEM((n, chans, rows), f32),
                pltpu.SemaphoreType.DMA((n,)),
            ],
            compiler_params=pltpu.CompilerParams(vmem_limit_bytes=VMEM_GRANT),
            name="finish",
        )(table, carry)
        return out.reshape(n * chans, rows)

    return jax.shard_map(
        local,
        mesh=mesh,
        in_specs=(P("dev", "grp"),),
        out_specs=P(None, ("grp", "dev")),
        check_vma=False,
    )
```

```python
import functools

import jax
import jax.numpy as jnp
from jax import lax
from jax.experimental import pallas as pl
from jax.experimental.pallas import tpu as pltpu
from jax.sharding import PartitionSpec as P

MESH = pl.DeviceIdType.MESH
LANES = 128
VMEM_GRANT = 46 << 20


def partner(me, k, n):
    if n & (n - 1):
        return lax.rem(me + k, n)
    other, bit = me, 1
    while bit < n:
        if k & bit:
            other = other + bit - 2 * bit * lax.rem(me // bit, 2)
        bit *= 2
    return other


def visit_order(n):
    return [*range(2, n, 2), *range(3, n, 2), *range(1, min(n, 2)), 0]


def greeting(n):
    if n & (n - 1) or n < 8:
        return list(range(1, n)), []
    across = (1 << (n.bit_length() - 2) // 2) - 1 << 1
    down = n - 2 - across
    near = [k for k in range(1, n) if not (k & across and k & down)]
    return near, [k for k in near if not k & (down | 1)]


def piece_spans(rows):
    cuts = [0, rows // 8, rows // 2, rows]
    return list(zip(cuts[:-1], cuts[1:]))


def kernel(n, groups, x_ref, t_ref, carry_ref, x_vm, s_vm, w_vm, run_vm, group_vm, give_vm,
           load_sem, send_sem, recv_sem, rsend_sem, rrecv_sem, csend_sem, crecv_sem, zsend_sem, zrecv_sem, ready_sem):
    me, grp = lax.axis_index("dev"), lax.axis_index("grp")
    chans, rows = t_ref.shape[1:]
    order = visit_order(n)
    spans = piece_spans(rows)
    others = {k: partner(me, k, n) for k in order}

    barrier = pltpu.get_barrier_semaphore()
    near, relays = greeting(n)
    for k in near:
        pl.semaphore_signal(barrier, inc=1, device_id={"dev": partner(me, k, n)}, device_id_type=MESH)

    @pl.when(grp > 0)
    def _():
        pl.semaphore_signal(barrier, inc=1, device_id={"grp": grp - 1}, device_id_type=MESH)

    @pl.when(grp < groups - 1)
    def _():
        pl.semaphore_signal(barrier, inc=1, device_id={"grp": grp + 1}, device_id_type=MESH)

    def load(piece, k):
        lo, hi = spans[piece]
        at = pl.ds(pl.multiple_of(others[k] * rows + lo, LANES), hi - lo)
        return pltpu.make_async_copy(x_ref.at[:, at], x_vm.at[:, at], load_sem.at[piece, k])

    for piece in range(len(spans)):
        for k in order:
            load(piece, k).start()

    shape = (2 * LANES, 2 * LANES)
    tile = min(rows // 8, 2048)
    steps = tile // LANES

    def scan(source, base, lo, hi, dest, run):
        def one(i, run):
            start = lo + i * tile
            block = source[:, pl.ds(pl.multiple_of(base + start, LANES), tile)]
            stack = jnp.concatenate(
                [block[:, j * LANES:(j + 1) * LANES] for j in range(steps)], axis=0)
            high = stack.astype(jnp.bfloat16)
            rest = stack - high.astype(jnp.float32)
            mid = rest.astype(jnp.bfloat16)
            low = (rest - mid.astype(jnp.float32)).astype(jnp.bfloat16)
            sums = jnp.dot(jnp.concatenate([high, mid], axis=1), w_vm[...],
                           preferred_element_type=jnp.float32)
            sums = sums + jnp.dot(low, w_vm[:LANES, :], preferred_element_type=jnp.float32)
            for j in range(steps):
                part = sums[j * chans:(j + 1) * chans]
                at = pl.ds(pl.multiple_of(start + j * LANES, LANES), LANES)
                dest[:, at] = part[:, :LANES] + run
                run = run + part[:, LANES:]
            return run

        return lax.fori_loop(0, (hi - lo) // tile, one, run)

    def raw(k, source):
        at = pl.ds(pl.multiple_of(others[k] * rows, LANES), spans[0][1])
        return pltpu.make_async_remote_copy(
            src_ref=x_vm.at[:, at], dst_ref=t_ref.at[source, :, pl.ds(0, spans[0][1])],
            send_sem=rsend_sem.at[others[k]], recv_sem=rrecv_sem.at[source],
            device_id={"dev": others[k]}, device_id_type=MESH)

    def send(piece, k):
        lo, hi = spans[piece]
        at = pl.ds(lo, hi - lo)
        pltpu.make_async_remote_copy(
            src_ref=s_vm.at[others[k], :, at], dst_ref=t_ref.at[me, :, at],
            send_sem=send_sem.at[others[k]], recv_sem=recv_sem.at[me],
            device_id={"dev": others[k]}, device_id_type=MESH).start()

    chained = jnp.where(grp > 0, 1, 0) + jnp.where(grp < groups - 1, 1, 0)
    pl.semaphore_wait(barrier, len(near) + chained)
    for k in relays:
        pl.semaphore_signal(ready_sem, inc=1, device_id={"dev": partner(me, k, n)}, device_id_type=MESH)
    met = False
    for k in [*(k for k in order if k in near), *(k for k in order if k not in near)]:
        if relays and not met and k not in near:
            pl.semaphore_wait(ready_sem, len(relays))
            met = True
        load(0, k).wait()
        if k:
            raw(k, me).start()

    row = lax.rem(lax.broadcasted_iota(jnp.int32, shape, 0), LANES)
    col = lax.broadcasted_iota(jnp.int32, shape, 1)
    w_vm[...] = jnp.where((row < col) | (col >= LANES), 1.0, 0.0).astype(jnp.bfloat16)
    run_vm[...] = jnp.zeros_like(run_vm)

    late = None
    for piece in range(len(spans)):
        for k in order:
            if piece:
                load(piece, k).wait()
            dest = s_vm.at[others[k]] if k else t_ref.at[me]
            run_vm[others[k]] = scan(x_vm, others[k] * rows, *spans[piece], dest, run_vm[others[k]])
            if late is not None:
                send(*late)
            late = (piece, k) if k and piece else None

    total = jnp.zeros((chans, LANES), jnp.float32)
    for j in range(n):
        give_vm[j] = total
        total = total + run_vm[j]

    def pass_on():
        return pltpu.make_async_remote_copy(
            src_ref=group_vm.at[1], dst_ref=group_vm.at[0], send_sem=zsend_sem, recv_sem=zrecv_sem,
            device_id={"grp": grp + 1}, device_id_type=MESH)

    @pl.when(grp == 0)
    def _():
        group_vm[0] = jnp.zeros_like(total)

    @pl.when(grp > 0)
    def _():
        pass_on().wait_recv()

    before = group_vm[0]
    group_vm[1] = before + total
    for j in range(n):
        give_vm[j] = give_vm[j] + before
    carry_ref[me] = give_vm[me]

    @pl.when(grp < groups - 1)
    def _():
        pass_on().start()

    def give(k, source):
        return pltpu.make_async_remote_copy(
            src_ref=give_vm.at[others[k]], dst_ref=carry_ref.at[source],
            send_sem=csend_sem.at[others[k]], recv_sem=crecv_sem.at[source],
            device_id={"dev": others[k]}, device_id_type=MESH)

    for k in order:
        if k:
            give(k, me).start()

    @pl.when(grp < groups - 1)
    def _():
        pass_on().wait_send()

    for k in order:
        if k:
            raw(k, others[k]).wait()
            block = t_ref.at[others[k]]
            scan(block, 0, *spans[0], block, jnp.zeros((chans, LANES), jnp.float32))

    rest = pl.ds(spans[0][1], rows - spans[0][1])
    for k in order:
        if k:
            pltpu.make_async_remote_copy(
                src_ref=s_vm.at[others[k], :, rest], dst_ref=t_ref.at[others[k], :, rest],
                send_sem=send_sem.at[others[k]], recv_sem=recv_sem.at[others[k]],
                device_id={"dev": others[k]}, device_id_type=MESH).wait()
            give(k, others[k]).wait()


def finish(n, t_ref, carry_ref, out_ref, stage, sem):
    rows = t_ref.shape[2]
    step = min(rows, 16 * LANES)

    def copy(j):
        return pltpu.make_async_copy(stage.at[j], out_ref.at[j], sem.at[j])

    for j in range(n):
        carry = carry_ref[j]
        wide = jnp.concatenate([carry] * (step // LANES), axis=1)

        def add(i, _):
            at = pl.ds(pl.multiple_of(i * step, LANES), step)
            stage[j, :, at] = t_ref[j, :, at] + wide
            return 0

        lax.fori_loop(0, rows // step, add, 0, unroll=True)
        copy(j).start()
    for j in range(n):
        copy(j).wait()


def solution(mesh):
    n, groups = mesh.shape["dev"], mesh.shape["grp"]

    def local(amounts):
        chans, length = amounts.shape
        rows = length // n
        f32 = jnp.float32
        table, carry = pl.pallas_call(
            functools.partial(kernel, n, groups),
            out_shape=[jax.ShapeDtypeStruct((n, chans, rows), f32),
                       jax.ShapeDtypeStruct((n, chans, LANES), f32)],
            in_specs=[pl.BlockSpec(memory_space=pl.ANY)],
            out_specs=[pl.BlockSpec(memory_space=pltpu.VMEM)] * 2,
            scratch_shapes=[
                pltpu.VMEM((chans, length), f32),
                pltpu.VMEM((n, chans, rows), f32),
                pltpu.VMEM((2 * LANES, 2 * LANES), jnp.bfloat16),
                pltpu.VMEM((n, chans, LANES), f32),
                pltpu.VMEM((2, chans, LANES), f32),
                pltpu.VMEM((n, chans, LANES), f32),
                pltpu.SemaphoreType.DMA((len(piece_spans(rows)), n)),
                pltpu.SemaphoreType.DMA((n,)),
                pltpu.SemaphoreType.DMA((n,)),
                pltpu.SemaphoreType.DMA((n,)),
                pltpu.SemaphoreType.DMA((n,)),
                pltpu.SemaphoreType.DMA((n,)),
                pltpu.SemaphoreType.DMA((n,)),
                pltpu.SemaphoreType.DMA,
                pltpu.SemaphoreType.DMA,
                pltpu.SemaphoreType.REGULAR,
            ],
            compiler_params=pltpu.CompilerParams(
                collective_id=0, has_side_effects=True, vmem_limit_bytes=VMEM_GRANT),
            name="exchange",
        )(amounts)
        out = pl.pallas_call(
            functools.partial(finish, n),
            out_shape=jax.ShapeDtypeStruct((n, chans, rows), f32),
            in_specs=[pl.BlockSpec(memory_space=pltpu.VMEM)] * 2,
            out_specs=pl.BlockSpec(memory_space=pl.ANY),
            scratch_shapes=[
                pltpu.VMEM((n, chans, rows), f32),
                pltpu.SemaphoreType.DMA((n,)),
            ],
            compiler_params=pltpu.CompilerParams(vmem_limit_bytes=VMEM_GRANT),
            name="finish",
        )(table, carry)
        return out.reshape(n * chans, rows)

    return jax.shard_map(
        local,
        mesh=mesh,
        in_specs=(P("dev", "grp"),),
        out_specs=P(None, ("grp", "dev")),
        check_vma=False,
    )
```
